32 devices in a mesh: dp: 16 (over z, x, core), rows: 2 (over y).
Axes of the slice: x: 2, y: 2, z: 4, core: 2. Of those that a mesh axis runs over, the one named last changes fastest.
Arguments:
- fine_level: bfloat16 [16, 32, 64, 256], P('dp', 'rows'), may hold values from -6 to 6
- out_grad: bfloat16 [16, 32, 64, 256], P('dp', 'rows'), may hold values from -6 to 6
- fine_input: bfloat16 [16, 32, 64, 256], P('dp', 'rows'), may hold values from -6 to 6
- mid_input: bfloat16 [16, 16, 32, 512], P('dp', None, None, 'rows'), may hold values from -6 to 6
- top_input: bfloat16 [16, 8, 16, 1024], P('dp', None, None, 'rows'), may hold values from -6 to 6
- smooth_weight: bfloat16 [3, 3, 256, 256], replicated, may hold values from -0.125 to 0.125
- fine_lateral: bfloat16 [256, 256], replicated, may hold values from -0.375 to 0.375
- mid_lateral: bfloat16 [512, 256], P('rows'), may hold values from -0.375 to 0.375
- top_lateral: bfloat16 [1024, 256], P('rows'), may hold values from -0.375 to 0.375
Outputs:
- grad_fine: bfloat16 [16, 32, 64, 256], P('dp', 'rows')
- grad_mid: bfloat16 [16, 16, 32, 512], P('dp', None, None, 'rows')
- grad_top: bfloat16 [16, 8, 16, 1024], P('dp', None, None, 'rows')
- kernel_grads: float32 [2560, 256], P('dp')
- midlat_grad: float32 [512, 256], P('rows')
- toplat_grad: float32 [1024, 256], P('rows')
The draws below stay inside these ranges and needn't reach their ends.
All inputs are finite; a program needn't handle non-finite values.
Results may differ from the reference program's by a relative error of at most 0.0062.
Values may be sent and summed in bfloat16 or wider, within the bound.
No kernel may reach another device: no remote copies, remote signals or barrier semaphores. Data moves between devices by JAX's collectives and lax.ppermute only.
A program may use at most 64 MiB of HBM per device.

```python
import jax
import jax.numpy as jnp
from jax import lax

FPN = 256
C2 = 256
C3 = 512
C4 = 1024
W2 = 64
BATCH = 16
H2 = 32
H3 = 16
W3 = 32
H4 = 8
W4 = 16


def block_levels(rng, extent, split, smallest, top_value):
    def one(axis_at, shards_of):
        draws = jax.random.uniform(jax.random.fold_in(jax.random.fold_in(rng, 6), axis_at), (shards_of,), jnp.float32, smallest / len(split), top_value / len(split))
        return jnp.repeat(jnp.exp(draws), extent[axis_at] // shards_of).reshape((-1,) + (1,) * (len(extent) - axis_at - 1))

    loudness = one(*split[0])
    for cut in split[1:]:
        loudness = loudness * one(*cut)
    return loudness


def scatter_about(stream_key, shape, spread, bound, cuts=(), held_as=jnp.bfloat16):
    level = block_levels(stream_key, shape, cuts, -0.22, 0.18) if cuts else 1.0
    result = jax.random.normal(stream_key, shape, jnp.float32) * spread * level
    return jnp.minimum(jnp.maximum(result, -bound), bound).astype(held_as)


def setup_inputs(seed: int = 0) -> dict:
    streams_of = jax.random.split(jax.random.key(seed), 10)
    fine_level = scatter_about(streams_of[0], (BATCH, H2, W2, FPN), 1.0, 6.0, ((0, 16), (1, 2)))
    out_grad = scatter_about(streams_of[1], (BATCH, H2, W2, FPN), 1.0, 6.0, ((0, 16), (1, 2)))
    fine_input = scatter_about(streams_of[2], (BATCH, H2, W2, C2), 1.0, 6.0, ((0, 16), (1, 2)))
    mid_input = scatter_about(streams_of[3], (BATCH, H3, W3, C3), 1.0, 6.0, ((0, 16), (3, 2)))
    top_input = scatter_about(streams_of[4], (BATCH, H4, W4, C4), 1.0, 6.0, ((0, 16), (3, 2)))
    smooth_weight = scatter_about(streams_of[5], (3, 3, FPN, FPN), (9 * FPN) ** -0.5, 0.125)
    fine_lateral = scatter_about(streams_of[6], (C2, FPN), FPN ** -0.5, 0.375)
    mid_lateral = scatter_about(streams_of[7], (C3, FPN), FPN ** -0.5, 0.375, ((0, 2),))
    top_lateral = scatter_about(streams_of[8], (C4, FPN), FPN ** -0.5, 0.375, ((0, 2),))
    return dict(fine_level=fine_level, out_grad=out_grad, fine_input=fine_input, mid_input=mid_input, top_input=top_input, smooth_weight=smooth_weight, fine_lateral=fine_lateral, mid_lateral=mid_lateral, top_lateral=top_lateral)


def pool_two(field):
    rows_n, cols_n, chans = field.shape
    return field.reshape(rows_n // 2, 2, cols_n // 2, 2, chans).sum(axis=(1, 3))


def contract_last(left, right):
    return lax.dot_general(left, right, (((1,), (1,)), ((), ())), preferred_element_type=jnp.float32)


def contract_first(left, right):
    return lax.dot_general(left, right, (((0,), (0,)), ((), ())), preferred_element_type=jnp.float32)


def one_image(fine_map, grad_map, fine_in, mid_in, top_in, smooth_weight, fine_lateral, mid_lateral, top_lateral):
    height, width, chans = grad_map.shape
    cells = height * width
    padded = jnp.pad(grad_map, ((1, 1), (1, 1), (0, 0)))
    fine_flat = fine_map.reshape(cells, chans)
    level_grad = jnp.zeros((cells, chans), jnp.float32)
    pieces = []
    for tap_a in range(3):
        for tap_b in range(3):
            shifted = padded[2 - tap_a:2 - tap_a + height, 2 - tap_b:2 - tap_b + width, :].reshape(cells, chans)
            level_grad = level_grad + contract_last(shifted, smooth_weight[tap_a, tap_b])
            pieces.append(contract_first(fine_flat, shifted))
    fine_grad = level_grad.astype(jnp.bfloat16)
    grad_fine = contract_last(fine_grad, fine_lateral).astype(jnp.bfloat16).reshape(height, width, -1)
    pieces.append(contract_first(fine_in.reshape(cells, -1), fine_grad))
    kernel_term = jnp.concatenate(pieces, axis=0)
    mid_grad = pool_two(level_grad.reshape(height, width, chans)).astype(jnp.bfloat16)
    top_grad = pool_two(mid_grad.astype(jnp.float32)).astype(jnp.bfloat16)
    mid_flat = mid_grad.reshape(-1, chans)
    top_flat = top_grad.reshape(-1, chans)
    grad_mid = contract_last(mid_flat, mid_lateral).astype(jnp.bfloat16).reshape(mid_in.shape)
    grad_top = contract_last(top_flat, top_lateral).astype(jnp.bfloat16).reshape(top_in.shape)
    mid_term = contract_first(mid_in.reshape(mid_flat.shape[0], -1), mid_flat)
    top_term = contract_first(top_in.reshape(top_flat.shape[0], -1), top_flat)
    return grad_fine, grad_mid, grad_top, kernel_term, mid_term, top_term


def reference(fine_level, out_grad, fine_input, mid_input, top_input, smooth_weight, fine_lateral, mid_lateral, top_lateral):
    def step(carry, items):
        outs = one_image(items[0], items[1], items[2], items[3], items[4], smooth_weight, fine_lateral, mid_lateral, top_lateral)
        carry = (carry[0] + outs[3], carry[1] + outs[4], carry[2] + outs[5])
        return carry, (outs[0], outs[1], outs[2])

    start = (jnp.zeros((9 * FPN + C2, FPN), jnp.float32), jnp.zeros((C3, FPN), jnp.float32), jnp.zeros((C4, FPN), jnp.float32))
    sums, grads = lax.scan(step, start, (fine_level, out_grad, fine_input, mid_input, top_input))
    return grads[0], grads[1], grads[2], sums[0], sums[1], sums[2]
```

```python
import jax
import jax.numpy as jnp
from jax import lax
from jax.experimental import pallas as pl
from jax.experimental.pallas import tpu as pltpu
from jax.sharding import PartitionSpec as P

BF = jnp.bfloat16
F32 = jnp.float32
VMEM = pl.BlockSpec(memory_space=pltpu.VMEM)
SMEM = pl.BlockSpec(memory_space=pltpu.SMEM)


def dot_last(left, right):
    return lax.dot_general(left, right, (((1,), (1,)), ((), ())), preferred_element_type=F32)


def dot_plain(left, right):
    return lax.dot_general(left, right, (((1,), (0,)), ((), ())), preferred_element_type=F32)


def pool_rows(source, target, lines, width):
    for line in range(lines // 2):
        pair = (
            source[pl.ds(2 * line * width, width), :]
            + source[pl.ds((2 * line + 1) * width, width), :]
        )
        for part in range(target.shape[0]):
            target[part, pl.ds(line * width, width), :] = pair[:, part * 128 : (part + 1) * 128]


def pool_cols(target):
    half = target.shape[1] // 2
    return jnp.concatenate(
        [
            target[part, pl.ds(0, half, stride=2), :] + target[part, pl.ds(1, half, stride=2), :]
            for part in range(target.shape[0])
        ],
        axis=1,
    )


def split_by_core(core, term, keep, send, chunk, chips):
    for chip in range(chips):
        own = pl.multiple_of((2 * chip + core) * chunk, 8)
        other = pl.multiple_of((2 * chip + 1 - core) * chunk, 8)
        keep[pl.ds(chip * chunk, chunk), :] = term[pl.ds(own, chunk), :].astype(keep.dtype)
        send[pl.ds(chip * chunk, chunk), :] = term[pl.ds(other, chunk), :].astype(send.dtype)


def fine_kernel(width, chunk, chips):
    def run(
        core, before, grad, after, level, fine_in, weight, lateral,
        grad_fine, keep, send, pooled,
        taps, term, level_grad, pairs,
    ):
        cells, chans = grad.shape
        lines = cells // width
        column = lax.broadcasted_iota(jnp.int32, (width, chans), 0)
        for line in range(lines + 2):
            if line == 0:
                here = before[...]
            elif line == lines + 1:
                here = after[...]
            else:
                here = grad[pl.ds((line - 1) * width, width), :]
            wide = here.astype(F32)
            nxt = jnp.where(column == width - 1, 0.0, pltpu.roll(wide, width - 1, 0))
            prv = jnp.where(column == 0, 0.0, pltpu.roll(wide, 1, 0))
            at = pl.ds(line * width, width)
            taps[at, 0:chans] = nxt.astype(BF)
            taps[at, chans : 2 * chans] = here
            taps[at, 2 * chans : 3 * chans] = prv.astype(BF)
        level_t = level[...].T
        total = None
        for tap in range(3):
            shifted = taps[pl.ds((2 - tap) * width, cells), :]
            wcat = jnp.concatenate([weight[tap, b] for b in range(3)], axis=1)
            part = dot_last(shifted, wcat)
            total = part if total is None else total + part
            row = dot_plain(level_t, shifted)
            for b in range(3):
                at = pl.ds((3 * tap + b) * chans, chans)
                term[at, :] = row[:, b * chans : (b + 1) * chans]
        level_grad[...] = total
        fine = total.astype(BF)
        grad_fine[...] = dot_last(fine, lateral[...]).astype(BF)
        term[pl.ds(9 * chans, fine_in.shape[1]), :] = dot_plain(fine_in[...].T, fine)
        split_by_core(core[0], term, keep, send, chunk, chips)
        pool_rows(level_grad, pairs, lines, width)
        pooled[...] = pool_cols(pairs).astype(BF)

    return run


def coarse_kernel(width, half):
    def run(
        core, mid_grad, mid_in, top_in, mid_lat, top_lat,
        grad_mid, grad_top, keep, send,
        term, wide, pairs,
    ):
        mid = mid_grad[...]
        wide[...] = mid.astype(F32)
        grad_mid[...] = dot_last(mid, mid_lat[...]).astype(BF)
        mids = mid_in.shape[1]
        term[pl.ds(0, mids), :] = dot_plain(mid_in[...].T, mid)
        pool_rows(wide, pairs, mid.shape[0] // width, width)
        top = pool_cols(pairs).astype(BF)
        grad_top[...] = dot_last(top, top_lat[...]).astype(BF)
        term[pl.ds(mids, top_in.shape[1]), :] = dot_plain(top_in[...].T, top)
        split_by_core(core[0], term, keep, send, half, 1)

    return run


def shape(*dims, dtype=BF):
    return jax.ShapeDtypeStruct(dims, dtype)


def scratch(*dims, dtype=F32):
    return pltpu.VMEM(dims, dtype)


def pick(array, index):
    return lax.dynamic_index_in_dim(array, index, 0, keepdims=False)


def body(
    fine_level,
    out_grad,
    fine_input,
    mid_input,
    top_input,
    smooth_weight,
    fine_lateral,
    mid_lateral,
    top_lateral,
):
    images, strip, width, chans = out_grad.shape
    assert images == 1
    cells = strip * width
    spread, tall = lax.axis_size("dp"), lax.axis_size("rows")
    chips, planes = spread // 2, spread // 4
    place, row = lax.axis_index("dp"), lax.axis_index("rows")
    core, side, plane = place % 2, (place // 2) % 2, place // 4
    core_arg = core.astype(jnp.int32).reshape(1)

    up = [(i, i + 1) for i in range(tall - 1)]
    down = [(j, i) for i, j in up]
    before = lax.ppermute(out_grad[0, strip - 1], "rows", up)
    after = lax.ppermute(out_grad[0, 0], "rows", down)

    rows_all = 9 * chans + fine_input.shape[3]
    chunk = rows_all // spread
    half_rows = chips * chunk
    grad_fine, keep, send, pooled = pl.pallas_call(
        fine_kernel(width, chunk, chips),
        out_shape=(
            shape(cells, fine_input.shape[3]),
            shape(half_rows, chans, dtype=F32),
            shape(half_rows, chans),
            shape(cells // 4, chans),
        ),
        in_specs=[SMEM] + [VMEM] * 7,
        out_specs=(VMEM,) * 4,
        scratch_shapes=[
            scratch((strip + 2) * width, 3 * chans, dtype=BF),
            scratch(rows_all, chans),
            scratch(cells, chans),
            scratch(chans // 128, cells // 2, 128),
        ],
        name="fine",
    )(
        core_arg,
        before,
        out_grad.reshape(cells, chans),
        after,
        fine_level.reshape(cells, chans),
        fine_input.reshape(cells, -1),
        smooth_weight,
        fine_lateral,
    )

    def swap_core(value):
        return lax.ppermute(value, "dp", [(i, i ^ 1) for i in range(spread)])

    if tall == 2:
        other = lax.ppermute(pooled, "rows", [(0, 1), (1, 0)])
        first = row == 0
        mid_grad = jnp.concatenate(
            [jnp.where(first, pooled, other), jnp.where(first, other, pooled)], axis=0
        )
    else:
        mid_grad = lax.all_gather(pooled, "rows", axis=0, tiled=True)

    got = swap_core(send)

    mids, tops = mid_input.shape[3], top_input.shape[3]
    mid_cells = mid_grad.shape[0]
    half = (mids + tops) // 2
    grad_mid, grad_top, keep_c, send_c = pl.pallas_call(
        coarse_kernel(width // 2, half),
        out_shape=(
            shape(mid_cells, mids),
            shape(mid_cells // 4, tops),
            shape(half, chans, dtype=F32),
            shape(half, chans),
        ),
        in_specs=[SMEM] + [VMEM] * 5,
        out_specs=(VMEM,) * 4,
        scratch_shapes=[
            scratch(mids + tops, chans),
            scratch(mid_cells, chans),
            scratch(chans // 128, mid_cells // 2, 128),
        ],
        name="coarse",
    )(
        core_arg,
        mid_grad,
        mid_input.reshape(mid_cells, mids),
        top_input.reshape(mid_cells // 4, tops),
        mid_lateral,
        top_lateral,
    )
    got_c = swap_core(send_c)

    sub = chunk // tall
    both = (keep + got.astype(F32)).reshape(planes, 2, tall, sub, chans)
    both = both.transpose(1, 2, 0, 3, 4).reshape(2 * tall, planes * sub, chans)
    total = pick(both, side * tall + row)
    arrived = []
    for move_side in range(2):
        for move_row in range(tall):
            if move_side or move_row:
                block = pick(both, (side ^ move_side) * tall + (row + move_row) % tall)
                pairs = []
                for d in range(spread):
                    for r in range(tall):
                        there = (d ^ (2 * move_side)) * tall + (r + move_row) % tall
                        pairs.append((d * tall + r, there))
                arrived.append(lax.ppermute(block.astype(BF), ("dp", "rows"), pairs))
    for value in arrived:
        total = total + value.astype(F32)
    total = total.reshape(planes, sub, chans)
    share = pick(total, plane)
    arrived = []
    for move in range(1, planes):
        block = pick(total, (plane + move) % planes).astype(BF)
        pairs = [(d, (d + 4 * move) % spread) for d in range(spread)]
        arrived.append(lax.ppermute(block, "dp", pairs))
    for value in arrived:
        share = share + value.astype(F32)
    if tall == 2:
        other = lax.ppermute(share, "rows", [(0, 1), (1, 0)])
        first = row == 0
        kernel_grads = jnp.concatenate(
            [jnp.where(first, share, other), jnp.where(first, other, share)], axis=0
        )
    else:
        kernel_grads = lax.all_gather(share, "rows", axis=0, tiled=True)

    piece = half // chips
    chip = place // 2
    both = (keep_c + got_c.astype(F32)).reshape(chips, piece, chans)
    total = pick(both, chip)
    arrived = []
    for move in range(1, chips):
        block = pick(both, (chip + move) % chips).astype(BF)
        pairs = [(d, (d + 2 * move) % spread) for d in range(spread)]
        arrived.append(lax.ppermute(block, "dp", pairs))
    for value in arrived:
        total = total + value.astype(F32)
    total = total.astype(BF)
    whole = [total]
    for move in range(1, chips):
        pairs = [(d, (d + 2 * move) % spread) for d in range(spread)]
        whole.append(lax.ppermute(total, "dp", pairs))
    whole = jnp.concatenate(whole[:1] + whole[:0:-1], axis=0)
    whole = lax.dynamic_slice_in_dim(
        jnp.concatenate([whole, whole], axis=0), (chips - chip) % chips * piece, half, axis=0
    )
    other = swap_core(whole)
    first = core == 0
    coarse = jnp.concatenate(
        [jnp.where(first, whole, other), jnp.where(first, other, whole)], axis=0
    ).astype(F32)

    return (
        grad_fine.reshape(fine_input.shape),
        grad_mid.reshape(mid_input.shape),
        grad_top.reshape(top_input.shape),
        kernel_grads,
        coarse[:mids],
        coarse[mids:],
    )


def solution(mesh):
    placed = (
        P("dp", "rows", None, None),
        P("dp", "rows", None, None),
        P("dp", "rows", None, None),
        P("dp", None, None, "rows"),
        P("dp", None, None, "rows"),
        P(),
        P(),
        P("rows", None),
        P("rows", None),
    )
    return jax.shard_map(
        body,
        mesh=mesh,
        in_specs=placed,
        out_specs=(
            P("dp", "rows", None, None),
            P("dp", None, None, "rows"),
            P("dp", None, None, "rows"),
            P("dp", None),
            P("rows", None),
            P("rows", None),
        ),
        check_vma=False,
    )
```

```python
import jax
import jax.numpy as jnp
from jax import lax
from jax.experimental import pallas as pl
from jax.experimental.pallas import tpu as pltpu
from jax.sharding import PartitionSpec as P


BF = jnp.bfloat16
F32 = jnp.float32
VMEM = pl.BlockSpec(memory_space=pltpu.VMEM)
SMEM = pl.BlockSpec(memory_space=pltpu.SMEM)


def dot_last(left, right):
    return lax.dot_general(left, right, (((1,), (1,)), ((), ())), preferred_element_type=F32)


def dot_plain(left, right):
    return lax.dot_general(left, right, (((1,), (0,)), ((), ())), preferred_element_type=F32)


def pool_rows(source, target, lines, width):
    for line in range(lines // 2):
        pair = (
            source[pl.ds(2 * line * width, width), :]
            + source[pl.ds((2 * line + 1) * width, width), :]
        )
        for part in range(target.shape[0]):
            target[part, pl.ds(line * width, width), :] = pair[:, part * 128 : (part + 1) * 128]


def pool_cols(target):
    half = target.shape[1] // 2
    return jnp.concatenate(
        [
            target[part, pl.ds(0, half, stride=2), :] + target[part, pl.ds(1, half, stride=2), :]
            for part in range(target.shape[0])
        ],
        axis=1,
    )


def level_kernel(width):
    def run(place, before, grad, after, weight, taps, fine, pooled, level_grad, pairs):
        cells, chans = grad.shape
        lines = cells // width
        column = lax.broadcasted_iota(jnp.int32, (width, chans), 0)
        for line in range(lines + 2):
            if line == 0:
                here = jnp.where(place[1] > 0, before[...].astype(F32), 0.0)
            elif line == lines + 1:
                here = jnp.where(place[2] > 0, after[...].astype(F32), 0.0)
            else:
                here = grad[pl.ds((line - 1) * width, width), :].astype(F32)
            nxt = jnp.where(column == width - 1, 0.0, pltpu.roll(here, width - 1, 0))
            prv = jnp.where(column == 0, 0.0, pltpu.roll(here, 1, 0))
            at = pl.ds(line * width, width)
            taps[at, 0:chans] = nxt.astype(BF)
            taps[at, chans : 2 * chans] = here.astype(BF)
            taps[at, 2 * chans : 3 * chans] = prv.astype(BF)
        total = None
        for tap in range(3):
            shifted = taps[pl.ds((2 - tap) * width, cells), :]
            wcat = jnp.concatenate([weight[tap, b] for b in range(3)], axis=1)
            part = dot_last(shifted, wcat)
            total = part if total is None else total + part
        level_grad[...] = total
        fine[...] = total.astype(BF)
        pool_rows(level_grad, pairs, lines, width)
        pooled[...] = pool_cols(pairs).astype(BF)

    return run


def weight_kernel(width, chips, tall, sub):
    def run(place, taps, fine, level, fine_in, *refs):
        term = refs[-1]
        cells, chans = fine.shape
        level_t = level[...].T
        for tap in range(3):
            row = dot_plain(level_t, taps[pl.ds((2 - tap) * width, cells), :])
            for b in range(3):
                at = pl.ds((3 * tap + b) * chans, chans)
                term[at, :] = row[:, b * chans : (b + 1) * chans]
        term[pl.ds(9 * chans, fine_in.shape[1]), :] = dot_plain(fine_in[...].T, fine[...])
        if len(refs) == 1:
            return
        keep, send = refs[:2]
        core = place[0]
        for chip in range(chips):
            for part in range(tall):
                to = pl.ds((part * chips + chip) * sub, sub)
                own = pl.multiple_of(((2 * chip + core) * tall + part) * sub, 8)
                other = pl.multiple_of(((2 * chip + 1 - core) * tall + part) * sub, 8)
                keep[to, :] = term[pl.ds(own, sub), :]
                send[to, :] = term[pl.ds(other, sub), :].astype(BF)

    return run


def grads_kernel(fine, mid, top, fine_lat, mid_lat, top_lat, grad_fine, grad_mid, grad_top):
    grad_fine[...] = dot_last(fine[...], fine_lat[...]).astype(BF)
    grad_mid[...] = dot_last(mid[...], mid_lat[...]).astype(BF)
    grad_top[...] = dot_last(top[...], top_lat[...]).astype(BF)


def coarse_kernel(width, half, blocks):
    def run(place, *refs):
        parts, (mid_in, top_in) = refs[:blocks], refs[blocks : blocks + 2]
        whole, top_out, keep, send, term, wide, pairs = refs[blocks + 2 :]
        count = parts[0].shape[0]
        spots = (place[3], 1 - place[3]) if blocks == 2 else (0,)
        for part, at in zip(parts, spots):
            whole[pl.ds(pl.multiple_of(at * count, 16), count), :] = part[...]
        mid = whole[...]
        wide[...] = mid.astype(F32)
        mids = mid_in.shape[1]
        term[pl.ds(0, mids), :] = dot_plain(mid_in[...].T, mid)
        pool_rows(wide, pairs, mid.shape[0] // width, width)
        top = pool_cols(pairs).astype(BF)
        top_out[...] = top
        term[pl.ds(mids, top_in.shape[1]), :] = dot_plain(top_in[...].T, top)
        core = place[0]
        own, other = pl.multiple_of(core * half, 8), pl.multiple_of((1 - core) * half, 8)
        keep[...] = term[pl.ds(own, half), :]
        send[...] = term[pl.ds(other, half), :].astype(BF)

    return run


def shape(*dims, dtype=BF):
    return jax.ShapeDtypeStruct(dims, dtype)


def scratch(*dims, dtype=F32):
    return pltpu.VMEM(dims, dtype)


def cost(flops):
    return pl.CostEstimate(flops=flops, bytes_accessed=0, transcendentals=0)


def pick(array, index):
    return lax.dynamic_index_in_dim(array, index, 0, keepdims=False)


def work(
    fine_level,
    out_grad,
    fine_input,
    mid_input,
    top_input,
    smooth_weight,
    fine_lateral,
    mid_lateral,
    top_lateral,
):
    images, strip, width, chans = out_grad.shape
    assert images == 1
    cells = strip * width
    spread, tall = lax.axis_size("dp"), lax.axis_size("rows")
    place, row = lax.axis_index("dp"), lax.axis_index("rows")
    core = place % 2
    chips = spread // 2
    there = jnp.stack([core, row > 0, row < tall - 1, row]).astype(jnp.int32)
    swap = [(0, 1), (1, 0)]

    def swap_core(value):
        return lax.ppermute(value, "dp", [(i, i ^ 1) for i in range(spread)])

    def join(index, mine, other):
        first = index == 0
        return jnp.concatenate(
            [jnp.where(first, mine, other), jnp.where(first, other, mine)], axis=0
        )

    flat = out_grad.reshape(cells, chans)
    top_line, low_line = flat[:width], flat[cells - width :]
    if tall == 2:
        before = after = lax.ppermute(jnp.where(row == 0, low_line, top_line), "rows", swap)
    else:
        up = [(i, i + 1) for i in range(tall - 1)]
        before = lax.ppermute(low_line, "rows", up)
        after = lax.ppermute(top_line, "rows", [(j, i) for i, j in up])

    taps, fine, pooled = pl.pallas_call(
        level_kernel(width),
        out_shape=(
            shape((strip + 2) * width, 3 * chans),
            shape(cells, chans),
            shape(cells // 4, chans),
        ),
        in_specs=[SMEM] + [VMEM] * 4,
        out_specs=(VMEM,) * 3,
        scratch_shapes=[scratch(cells, chans), scratch(chans // 128, cells // 2, 128)],
        cost_estimate=cost(18 * cells * chans * chans),
        name="level",
    )(there, before, flat, after, smooth_weight)

    if tall == 2:
        blocks = (pooled, lax.ppermute(pooled, "rows", swap))
    else:
        blocks = (lax.all_gather(pooled, "rows", axis=0, tiled=True),)

    rows_all = 9 * chans + fine_input.shape[3]
    sub = rows_all // (spread * tall)
    half_rows = rows_all // 2
    aligned = sub % 8 == 0
    whole_term = shape(rows_all, chans, dtype=F32)
    halves = (shape(half_rows, chans, dtype=F32), shape(half_rows, chans))
    out = pl.pallas_call(
        weight_kernel(width, chips, tall, sub),
        out_shape=halves if aligned else (whole_term,),
        in_specs=[SMEM] + [VMEM] * 4,
        out_specs=(VMEM,) * (2 if aligned else 1),
        scratch_shapes=[scratch(rows_all, chans)] if aligned else [],
        cost_estimate=cost(20 * cells * chans * chans),
        name="weights",
    )(
        there,
        taps,
        fine,
        fine_level.reshape(cells, chans),
        fine_input.reshape(cells, -1),
    )
    if aligned:
        keep, send = out
    else:
        term = out[0].reshape(chips, 2, tall, sub, chans).transpose(1, 2, 0, 3, 4)
        term = term.reshape(2, half_rows, chans)
        keep, send = pick(term, core), pick(term, 1 - core).astype(BF)
    got = swap_core(send)

    both = (keep + got.astype(F32)).reshape(tall, chips * sub, chans)
    fine_sum = pick(both, row)
    for move in range(1, tall):
        block = pick(both, (row + move) % tall).astype(BF)
        pairs = [(r, (r + move) % tall) for r in range(tall)]
        moved = lax.ppermute(block, "rows", pairs)
        fine_sum = fine_sum + moved.astype(F32)

    mids, tops = mid_input.shape[3], top_input.shape[3]
    mid_cells = mid_input.shape[1] * mid_input.shape[2]
    half = (mids + tops) // 2
    mid_grad, top_grad, keep, send = pl.pallas_call(
        coarse_kernel(width // 2, half, len(blocks)),
        out_shape=(
            shape(mid_cells, chans),
            shape(mid_cells // 4, chans),
            shape(half, chans, dtype=F32),
            shape(half, chans),
        ),
        in_specs=[SMEM] + [VMEM] * (2 + len(blocks)),
        out_specs=(VMEM,) * 4,
        scratch_shapes=[
            scratch(mids + tops, chans),
            scratch(mid_cells, chans),
            scratch(chans // 128, mid_cells // 2, 128),
        ],
        cost_estimate=cost(2 * mid_cells * chans * (mids + tops // 4)),
        name="coarse",
    )(there, *blocks, mid_input.reshape(mid_cells, mids), top_input.reshape(mid_cells // 4, tops))
    coarse_sum = keep + swap_core(send).astype(F32)

    grad_fine, grad_mid, grad_top = pl.pallas_call(
        grads_kernel,
        out_shape=(
            shape(cells, fine_input.shape[3]),
            shape(mid_cells, mids),
            shape(mid_cells // 4, tops),
        ),
        in_specs=[VMEM] * 6,
        out_specs=(VMEM,) * 3,
        cost_estimate=cost(4 * cells * chans * chans),
        name="grads",
    )(fine, mid_grad, top_grad, fine_lateral, mid_lateral, top_lateral)

    piece = half // chips
    groups = [[2 * k + c for k in range(chips)] for c in range(2)]
    packed = jnp.concatenate(
        [
            fine_sum.reshape(chips, sub, chans).astype(BF),
            coarse_sum.reshape(chips, piece, chans).astype(BF),
        ],
        axis=1,
    )
    packed = lax.all_to_all(packed, "dp", 0, 0, tiled=True, axis_index_groups=groups)
    share = packed[:, :sub].astype(F32).sum(axis=0)
    part = packed[:, sub:].astype(F32).sum(axis=0).astype(BF)

    if tall == 2:
        kernel_grads = join(row, share, lax.ppermute(share, "rows", swap))
    else:
        kernel_grads = lax.all_gather(share, "rows", axis=0, tiled=True)

    part = jnp.broadcast_to(part[None], (chips, piece, chans))
    part = lax.all_to_all(part, "dp", 0, 0, tiled=True, axis_index_groups=groups)
    part = part.reshape(half, chans)
    coarse = join(core, part, swap_core(part)).astype(F32)

    return (
        grad_fine.reshape(fine_input.shape),
        grad_mid.reshape(mid_input.shape),
        grad_top.reshape(top_input.shape),
        kernel_grads,
        coarse[:mids],
        coarse[mids:],
    )


def solution(mesh):
    placed = (
        P("dp", "rows", None, None),
        P("dp", "rows", None, None),
        P("dp", "rows", None, None),
        P("dp", None, None, "rows"),
        P("dp", None, None, "rows"),
        P(),
        P(),
        P("rows", None),
        P("rows", None),
    )
    return jax.shard_map(
        work,
        mesh=mesh,
        in_specs=placed,
        out_specs=(
            P("dp", "rows", None, None),
            P("dp", None, None, "rows"),
            P("dp", None, None, "rows"),
            P("dp", None),
            P("rows", None),
            P("rows", None),
        ),
        check_vma=False,
    )
```

```python
import jax
import jax.numpy as jnp
from jax import lax
from jax.experimental import pallas as pl
from jax.experimental.pallas import tpu as pltpu
from jax.sharding import PartitionSpec as P


BF = jnp.bfloat16
F32 = jnp.float32
VMEM = pl.BlockSpec(memory_space=pltpu.VMEM)
SMEM = pl.BlockSpec(memory_space=pltpu.SMEM)


def dot_last(left, right):
    return lax.dot_general(left, right, (((1,), (1,)), ((), ())), preferred_element_type=F32)


def dot_plain(left, right):
    return lax.dot_general(left, right, (((1,), (0,)), ((), ())), preferred_element_type=F32)


def pool_rows(source, target, lines, width):
    for line in range(lines // 2):
        pair = (
            source[pl.ds(2 * line * width, width), :]
            + source[pl.ds((2 * line + 1) * width, width), :]
        )
        for part in range(target.shape[0]):
            target[part, pl.ds(line * width, width), :] = pair[:, part * 128 : (part + 1) * 128]


def pool_cols(target):
    half = target.shape[1] // 2
    return jnp.concatenate(
        [
            target[part, pl.ds(0, half, stride=2), :] + target[part, pl.ds(1, half, stride=2), :]
            for part in range(target.shape[0])
        ],
        axis=1,
    )


def level_kernel(width):
    def run(place, before, grad, after, weight, taps, fine, pooled, level_grad, pairs):
        cells, chans = grad.shape
        lines = cells // width
        column = lax.broadcasted_iota(jnp.int32, (width, chans), 0)
        for line in range(lines + 2):
            if line == 0:
                here = jnp.where(place[1] > 0, before[...].astype(F32), 0.0)
            elif line == lines + 1:
                here = jnp.where(place[2] > 0, after[...].astype(F32), 0.0)
            else:
                here = grad[pl.ds((line - 1) * width, width), :].astype(F32)
            nxt = jnp.where(column == width - 1, 0.0, pltpu.roll(here, width - 1, 0))
            prv = jnp.where(column == 0, 0.0, pltpu.roll(here, 1, 0))
            at = pl.ds(line * width, width)
            taps[at, 0:chans] = nxt.astype(BF)
            taps[at, chans : 2 * chans] = here.astype(BF)
            taps[at, 2 * chans : 3 * chans] = prv.astype(BF)
        total = None
        for tap in range(3):
            shifted = taps[pl.ds((2 - tap) * width, cells), :]
            wcat = jnp.concatenate([weight[tap, b] for b in range(3)], axis=1)
            part = dot_last(shifted, wcat)
            total = part if total is None else total + part
        level_grad[...] = total
        fine[...] = total.astype(BF)
        pool_rows(level_grad, pairs, lines, width)
        pooled[...] = pool_cols(pairs).astype(BF)

    return run


def weight_kernel(width, chips, tall, sub):
    def run(place, taps, fine, level, fine_in, *refs):
        term = refs[-1]
        cells, chans = fine.shape
        level_t = level[...].T
        for tap in range(3):
            row = dot_plain(level_t, taps[pl.ds((2 - tap) * width, cells), :])
            for b in range(3):
                at = pl.ds((3 * tap + b) * chans, chans)
                term[at, :] = row[:, b * chans : (b + 1) * chans]
        term[pl.ds(9 * chans, fine_in.shape[1]), :] = dot_plain(fine_in[...].T, fine[...])
        if len(refs) == 1:
            return
        keep, send = refs[:2]
        core = place[0]
        for chip in range(chips):
            for part in range(tall):
                to = pl.ds((part * chips + chip) * sub, sub)
                own = pl.multiple_of(((2 * chip + core) * tall + part) * sub, 8)
                other = pl.multiple_of(((2 * chip + 1 - core) * tall + part) * sub, 8)
                keep[to, :] = term[pl.ds(own, sub), :]
                send[to, :] = term[pl.ds(other, sub), :].astype(BF)

    return run


def grads_kernel(fine, mid, top, fine_lat, mid_lat, top_lat, grad_fine, grad_mid, grad_top):
    grad_fine[...] = dot_last(fine[...], fine_lat[...]).astype(BF)
    grad_mid[...] = dot_last(mid[...], mid_lat[...]).astype(BF)
    grad_top[...] = dot_last(top[...], top_lat[...]).astype(BF)


def coarse_kernel(width, half, blocks):
    def run(place, *refs):
        parts, (mid_in, top_in) = refs[:blocks], refs[blocks : blocks + 2]
        whole, top_out, keep, send, term, wide, pairs = refs[blocks + 2 :]
        count = parts[0].shape[0]
        spots = (place[3], 1 - place[3]) if blocks == 2 else (0,)
        for part, at in zip(parts, spots):
            whole[pl.ds(pl.multiple_of(at * count, 16), count), :] = part[...]
        mid = whole[...]
        wide[...] = mid.astype(F32)
        mids = mid_in.shape[1]
        term[pl.ds(0, mids), :] = dot_plain(mid_in[...].T, mid)
        pool_rows(wide, pairs, mid.shape[0] // width, width)
        top = pool_cols(pairs).astype(BF)
        top_out[...] = top
        term[pl.ds(mids, top_in.shape[1]), :] = dot_plain(top_in[...].T, top)
        core = place[0]
        own, other = pl.multiple_of(core * half, 8), pl.multiple_of((1 - core) * half, 8)
        keep[...] = term[pl.ds(own, half), :]
        send[...] = term[pl.ds(other, half), :].astype(BF)

    return run


def finish_kernel(place, mine, other, mids, tops):
    own, far = mine[...].astype(F32), other[...].astype(F32)
    first = place[0] == 0
    whole = jnp.concatenate([jnp.where(first, own, far), jnp.where(first, far, own)], axis=0)
    count = mids.shape[0]
    mids[...] = whole[:count]
    tops[...] = whole[count:]


def shape(*dims, dtype=BF):
    return jax.ShapeDtypeStruct(dims, dtype)


def scratch(*dims, dtype=F32):
    return pltpu.VMEM(dims, dtype)


def cost(flops):
    return pl.CostEstimate(flops=flops, bytes_accessed=0, transcendentals=0)


def pick(array, index):
    return lax.dynamic_index_in_dim(array, index, 0, keepdims=False)


def work(
    fine_level,
    out_grad,
    fine_input,
    mid_input,
    top_input,
    smooth_weight,
    fine_lateral,
    mid_lateral,
    top_lateral,
):
    images, strip, width, chans = out_grad.shape
    assert images == 1
    cells = strip * width
    spread, tall = lax.axis_size("dp"), lax.axis_size("rows")
    place, row = lax.axis_index("dp"), lax.axis_index("rows")
    core = place % 2
    chips = spread // 2
    there = jnp.stack([core, row > 0, row < tall - 1, row]).astype(jnp.int32)
    swap = [(0, 1), (1, 0)]

    def swap_core(value):
        return lax.ppermute(value, "dp", [(i, i ^ 1) for i in range(spread)])

    def join(index, mine, other):
        first = index == 0
        return jnp.concatenate(
            [jnp.where(first, mine, other), jnp.where(first, other, mine)], axis=0
        )

    flat = out_grad.reshape(cells, chans)
    top_line, low_line = flat[:width], flat[cells - width :]
    if tall == 2:
        before = after = lax.ppermute(jnp.where(row == 0, low_line, top_line), "rows", swap)
    else:
        up = [(i, i + 1) for i in range(tall - 1)]
        before = lax.ppermute(low_line, "rows", up)
        after = lax.ppermute(top_line, "rows", [(j, i) for i, j in up])

    taps, fine, pooled = pl.pallas_call(
        level_kernel(width),
        out_shape=(
            shape((strip + 2) * width, 3 * chans),
            shape(cells, chans),
            shape(cells // 4, chans),
        ),
        in_specs=[SMEM] + [VMEM] * 4,
        out_specs=(VMEM,) * 3,
        scratch_shapes=[scratch(cells, chans), scratch(chans // 128, cells // 2, 128)],
        cost_estimate=cost(18 * cells * chans * chans),
        name="level",
    )(there, before, flat, after, smooth_weight)

    if tall == 2:
        blocks = (pooled, lax.ppermute(pooled, "rows", swap))
    else:
        blocks = (lax.all_gather(pooled, "rows", axis=0, tiled=True),)

    rows_all = 9 * chans + fine_input.shape[3]
    sub = rows_all // (spread * tall)
    half_rows = rows_all // 2
    aligned = sub % 8 == 0
    whole_term = shape(rows_all, chans, dtype=F32)
    halves = (shape(half_rows, chans, dtype=F32), shape(half_rows, chans))
    out = pl.pallas_call(
        weight_kernel(width, chips, tall, sub),
        out_shape=halves if aligned else (whole_term,),
        in_specs=[SMEM] + [VMEM] * 4,
        out_specs=(VMEM,) * (2 if aligned else 1),
        scratch_shapes=[scratch(rows_all, chans)] if aligned else [],
        cost_estimate=cost(20 * cells * chans * chans),
        name="weights",
    )(
        there,
        taps,
        fine,
        fine_level.reshape(cells, chans),
        fine_input.reshape(cells, -1),
    )
    if aligned:
        keep, send = out
    else:
        term = out[0].reshape(chips, 2, tall, sub, chans).transpose(1, 2, 0, 3, 4)
        term = term.reshape(2, half_rows, chans)
        keep, send = pick(term, core), pick(term, 1 - core).astype(BF)
    got = swap_core(send)

    keep, got = (value.reshape(tall, chips * sub, chans) for value in (keep, got))

    def pair_sum(index):
        return pick(keep, index) + pick(got, index).astype(F32)

    fine_sum = pair_sum(row)
    for move in range(1, tall):
        block = pair_sum((row + move) % tall).astype(BF)
        pairs = [(r, (r + move) % tall) for r in range(tall)]
        moved = lax.ppermute(block, "rows", pairs)
        fine_sum = fine_sum + moved.astype(F32)

    mids, tops = mid_input.shape[3], top_input.shape[3]
    mid_cells = mid_input.shape[1] * mid_input.shape[2]
    half = (mids + tops) // 2
    mid_grad, top_grad, keep, send = pl.pallas_call(
        coarse_kernel(width // 2, half, len(blocks)),
        out_shape=(
            shape(mid_cells, chans),
            shape(mid_cells // 4, chans),
            shape(half, chans, dtype=F32),
            shape(half, chans),
        ),
        in_specs=[SMEM] + [VMEM] * (2 + len(blocks)),
        out_specs=(VMEM,) * 4,
        scratch_shapes=[
            scratch(mids + tops, chans),
            scratch(mid_cells, chans),
            scratch(chans // 128, mid_cells // 2, 128),
        ],
        cost_estimate=cost(2 * mid_cells * chans * (mids + tops // 4)),
        name="coarse",
    )(there, *blocks, mid_input.reshape(mid_cells, mids), top_input.reshape(mid_cells // 4, tops))
    coarse_sum = keep + swap_core(send).astype(F32)

    grad_fine, grad_mid, grad_top = pl.pallas_call(
        grads_kernel,
        out_shape=(
            shape(cells, fine_input.shape[3]),
            shape(mid_cells, mids),
            shape(mid_cells // 4, tops),
        ),
        in_specs=[VMEM] * 6,
        out_specs=(VMEM,) * 3,
        cost_estimate=cost(4 * cells * chans * chans),
        name="grads",
    )(fine, mid_grad, top_grad, fine_lateral, mid_lateral, top_lateral)

    piece = half // chips
    groups = [[2 * k + c for k in range(chips)] for c in range(2)]
    packed = jnp.concatenate(
        [
            fine_sum.reshape(chips, sub, chans).astype(BF),
            coarse_sum.reshape(chips, piece, chans).astype(BF),
        ],
        axis=1,
    )
    packed = lax.all_to_all(packed, "dp", 0, 0, tiled=True, axis_index_groups=groups)
    share = packed[:, :sub].astype(F32).sum(axis=0)
    part = packed[:, sub:].astype(F32).sum(axis=0).astype(BF)

    if tall == 2:
        kernel_grads = join(row, share, lax.ppermute(share, "rows", swap))
    else:
        kernel_grads = lax.all_gather(share, "rows", axis=0, tiled=True)

    part = jnp.broadcast_to(part[None], (chips, piece, chans))
    part = lax.all_to_all(part, "dp", 0, 0, tiled=True, axis_index_groups=groups)
    part = part.reshape(half, chans)
    midlat_grad, toplat_grad = pl.pallas_call(
        finish_kernel,
        out_shape=(shape(mids, chans, dtype=F32), shape(tops, chans, dtype=F32)),
        in_specs=[SMEM, VMEM, VMEM],
        out_specs=(VMEM,) * 2,
        name="finish",
    )(there, part, swap_core(part))

    return (
        grad_fine.reshape(fine_input.shape),
        grad_mid.reshape(mid_input.shape),
        grad_top.reshape(top_input.shape),
        kernel_grads,
        midlat_grad,
        toplat_grad,
    )


def solution(mesh):
    placed = (
        P("dp", "rows", None, None),
        P("dp", "rows", None, None),
        P("dp", "rows", None, None),
        P("dp", None, None, "rows"),
        P("dp", None, None, "rows"),
        P(),
        P(),
        P("rows", None),
        P("rows", None),
    )
    return jax.shard_map(
        work,
        mesh=mesh,
        in_specs=placed,
        out_specs=(
            P("dp", "rows", None, None),
            P("dp", None, None, "rows"),
            P("dp", None, None, "rows"),
            P("dp", None),
            P("rows", None),
            P("rows", None),
        ),
        check_vma=False,
    )
```
